32 devices in a mesh: leaf: 32 (over z, y, x, core).
Axes of the slice: x: 2, y: 2, z: 4, core: 2. Of those that a mesh axis runs over, the one named last changes fastest.
Arguments:
- panels: bfloat16 [64, 64, 256], P('leaf'), may hold values from -6 to 6
- basis: bfloat16 [64, 64, 256], P('leaf'), may hold values from -0.375 to 0.375
- transfer: bfloat16 [64, 64, 64], P('leaf'), may hold values from -0.25 to 0.25
- near_blocks: bfloat16 [64, 27, 256, 256], P('leaf'), may hold values from -0.078125 to 0.078125
- coupling: bfloat16 [2, 343, 4096], replicated, may hold values from -0.0546875 to 0.0546875
- near_list: int32 [64, 27], P('leaf'), may hold values from -1 to 63, as said below
Outputs:
- product: bfloat16 [64, 64, 256], P('leaf')
The draws below stay inside these ranges and needn't reach their ends.
Inputs may be any that keep to these rules, and one draw needn't show every extreme that they name: `near_list`: row i lists, in an order of no meaning, leaf i and the leaves whose grid positions differ from it by at most one in each coordinate; -1 fills the other slots.
All inputs are finite; a program needn't handle non-finite values.
Results may differ from the reference program's by a relative error of at most 0.0035.
Values may be sent and summed in bfloat16 or wider, within the bound.
A program may use at most 192 MiB of HBM per device.

```python
import jax
import jax.numpy as jnp
from jax import lax

LEAF = 256
RANK = 64
COLS = 64
NNEAR = 27
SHIFTS = 343
LEAVES = 64
CLUSTERS = 8


def decode_drawn(indices, bit_count):
    coords = [jnp.zeros_like(indices) for a in range(3)]
    for k in range(bit_count):
        coords[k % 3] = coords[k % 3] + ((indices >> k & 1) << k // 3)
    return coords


def encode_drawn(coords, bit_count):
    result = jnp.zeros_like(coords[0])
    for k in range(bit_count):
        result = result + ((coords[k % 3] >> k // 3 & 1) << k)
    return result


def grid_extent_drawn(bit_count):
    return [2 ** len([k for k in range(bit_count) if k % 3 == a]) for a in range(3)]


def shuffle_rows(key, table, width):
    column = jnp.arange(table.shape[1], dtype=jnp.int32)[None, :]
    noise = jax.random.randint(key, table.shape, 0, 1 << 20, dtype=jnp.int32)
    score = jnp.where(table >= 0, 1 << 29, 0) + noise * 256 + column
    order = jnp.argsort(-score, axis=1)
    return jnp.take_along_axis(table, order, axis=1)[:, :width].astype(jnp.int32)


def near_rows(key, bit_count):
    count = 2 ** bit_count
    coords = decode_drawn(jnp.arange(count, dtype=jnp.int32), bit_count)
    extent = grid_extent_drawn(bit_count)
    entries = []
    for delta in [(a, b, c) for a in (-1, 0, 1) for b in (-1, 0, 1) for c in (-1, 0, 1)]:
        moved = [coords[a] + delta[a] for a in range(3)]
        inside = (moved[0] >= 0) & (moved[0] < extent[0]) & (moved[1] >= 0) & (moved[1] < extent[1]) & (moved[2] >= 0) & (moved[2] < extent[2])
        entries.append(jnp.where(inside, encode_drawn(moved, bit_count), -1))
    return shuffle_rows(key, jnp.stack(entries, axis=1), NNEAR)


def draw_near_list(key, part):
    return near_rows(jax.random.fold_in(key, 11), int(LEAVES).bit_length() - 1)


def levels(rng, shape, cuts, smallest, largest):
    level = 1.0
    for dim, shards_of in cuts:
        heights = jax.random.uniform(jax.random.fold_in(jax.random.fold_in(rng, 6), dim), (shards_of,), jnp.float32, smallest / len(cuts), largest / len(cuts))
        level = level * jnp.repeat(jnp.exp(heights), shape[dim] // shards_of).reshape((-1,) + (1,) * (len(shape) - 1 - dim))
    return level


def centred(stream_key, shape, spread, bound, split=(), kind=jnp.bfloat16):
    loudness = levels(stream_key, shape, split, -0.22, 0.18) if split else 1.0
    values = jax.random.normal(stream_key, shape, jnp.float32) * spread * loudness
    return jnp.minimum(jnp.maximum(values, -bound), bound).astype(kind)


def setup_inputs(seed: int = 0) -> dict:
    streams_of = jax.random.split(jax.random.key(seed), 7)
    return {
        "panels": centred(streams_of[0], (LEAVES, COLS, LEAF), 1.0, 6.0, ((0, 32),)),
        "basis": centred(streams_of[1], (LEAVES, RANK, LEAF), LEAF ** -0.5, 0.375, ((0, 32),)),
        "transfer": centred(streams_of[2], (LEAVES, RANK, RANK), (8 * RANK) ** -0.5, 0.25, ((0, 32),)),
        "near_blocks": centred(streams_of[3], (LEAVES, NNEAR, LEAF, LEAF), (NNEAR * LEAF) ** -0.5, 0.078125, ((0, 32),)),
        "coupling": centred(streams_of[4], (2, SHIFTS, RANK * RANK), (189 * RANK) ** -0.5, 0.0546875),
        "near_list": draw_near_list(jax.random.fold_in(streams_of[6], 71), 0),
    }


def decode(indices, bit_count):
    coords = [jnp.zeros_like(indices) for a in range(3)]
    for k in range(bit_count):
        coords[k % 3] = coords[k % 3] + (((indices >> k) & 1) << (k // 3))
    return coords


def encode(coords, bit_count):
    result = jnp.zeros_like(coords[0])
    for k in range(bit_count):
        result = result + (((coords[k % 3] >> (k // 3)) & 1) << k)
    return result


def grid_extent(bit_count):
    return [2 ** len([k for k in range(bit_count) if k % 3 == a]) for a in range(3)]


def far_table(cells, bit_count):
    coords = decode(cells, bit_count)
    extent = grid_extent(bit_count)
    entries = []
    for delta in [(a, b, c) for a in (-1, 0, 1) for b in (-1, 0, 1) for c in (-1, 0, 1)]:
        upper = [(coords[a] >> 1) + delta[a] for a in range(3)]
        inside = (upper[0] >= 0) & (upper[0] < extent[0] // 2) & (upper[1] >= 0) & (upper[1] < extent[1] // 2) & (upper[2] >= 0) & (upper[2] < extent[2] // 2)
        for child in [(a, b, c) for a in (0, 1) for b in (0, 1) for c in (0, 1)]:
            moved = [2 * upper[a] + child[a] for a in range(3)]
            apart = (jnp.abs(moved[0] - coords[0]) > 1) | (jnp.abs(moved[1] - coords[1]) > 1) | (jnp.abs(moved[2] - coords[2]) > 1)
            entries.append(jnp.where(inside & apart, encode(moved, bit_count), -1))
    return jnp.stack(entries, axis=-1).astype(jnp.int32)


def shift_code(targets, sources, bit_count):
    safe = jnp.maximum(sources, 0)
    first = decode(targets, bit_count)
    second = decode(safe, bit_count)
    return (49 * (second[0] - first[0] + 3) + 7 * (second[1] - first[1] + 3) + (second[2] - first[2] + 3)).astype(jnp.int32)


def couple(coef_table, table, rows, codes):
    valid = (rows >= 0).astype(jnp.float32)
    picked = jnp.take(coef_table, jnp.maximum(rows, 0), axis=0).astype(jnp.float32) * valid[:, None, None]
    mats = jnp.take(table, codes, axis=0).astype(jnp.float32).reshape(rows.shape[0], RANK, RANK)
    return jnp.einsum('jcr,jrs->cs', picked, mats)


def reference(panels, basis, transfer, near_blocks, coupling, near_list):
    bit_count = int(LEAVES).bit_length() - 1
    leaf_coef = jnp.einsum('lcq,lrq->lcr', panels.astype(jnp.float32), basis.astype(jnp.float32)).astype(jnp.bfloat16)
    partial_value = jnp.einsum('lcr,lrs->lcs', leaf_coef.astype(jnp.float32), transfer.astype(jnp.float32))
    cluster_coef = partial_value.reshape(CLUSTERS, 8, COLS, RANK).sum(axis=1).astype(jnp.bfloat16)
    leaf_ids = jnp.arange(LEAVES, dtype=jnp.int32)
    cluster_ids = jnp.arange(CLUSTERS, dtype=jnp.int32)
    far_leaf = far_table(leaf_ids, bit_count)
    far_cluster = far_table(cluster_ids, bit_count - 3)
    codes_leaf = shift_code(leaf_ids[:, None], far_leaf, bit_count)
    codes_cluster = shift_code(cluster_ids[:, None], far_cluster, bit_count - 3)
    down_coef = lax.map(lambda item: couple(cluster_coef, coupling[1], item[0], item[1]), (far_cluster, codes_cluster)).astype(jnp.bfloat16)
    leaf_far = lax.map(lambda item: couple(leaf_coef, coupling[0], item[0], item[1]), (far_leaf, codes_leaf))
    parent_down = jnp.repeat(down_coef, 8, axis=0).astype(jnp.float32)
    far_coef = (leaf_far + jnp.einsum('lcs,lrs->lcr', parent_down, transfer.astype(jnp.float32))).astype(jnp.bfloat16)
    far_term = jnp.einsum('lcr,lrq->lcq', far_coef.astype(jnp.float32), basis.astype(jnp.float32))

    def near_one(item):
        rows, blocks = item
        valid = (rows >= 0).astype(jnp.float32)
        picked = jnp.take(panels, jnp.maximum(rows, 0), axis=0).astype(jnp.float32) * valid[:, None, None]
        return jnp.einsum('kcq,kqp->cp', picked, blocks.astype(jnp.float32))

    near = lax.map(near_one, (near_list, near_blocks))
    return (near + far_term).astype(jnp.bfloat16)
```

```python
import functools

import jax
import jax.numpy as jnp
from jax import lax
from jax.experimental import pallas as pl
from jax.experimental.pallas import tpu as pltpu
from jax.sharding import PartitionSpec as P

MESH = pl.DeviceIdType.MESH
F32 = jnp.float32
BF16 = jnp.bfloat16
REACH = 3
SPAN = 2 * REACH + 1
TN = (((0,), (0,)), ((), ()))
NT = (((1,), (1,)), ((), ()))
OFFSETS = [(a, b, c) for a in (-1, 0, 1) for b in (-1, 0, 1) for c in (-1, 0, 1)]


def axis_bits(first, bit_count):
    return [[b for b in range(bit_count) if (b + first) % 3 == a] for a in range(3)]


def coords_of(index, bits):
    return [
        sum(((index // 2**b) % 2) * 2**p for p, b in enumerate(bits[a])) + index * 0
        for a in range(3)
    ]


def index_of(coords, bits):
    return sum(((coords[a] // 2**p) % 2) * 2**b for a in range(3) for p, b in enumerate(bits[a]))


def inside(coords, bits):
    ok = None
    for a in range(3):
        here = (coords[a] >= 0) & (coords[a] < 2 ** len(bits[a]))
        ok = here if ok is None else ok & here
    return ok


def far_sum(targets, bit_count, stacked, table, pitch, rank):
    half = rank // 2
    bits = axis_bits(0, bit_count - 3)
    count = 2 ** (bit_count - 3)
    home = [c // 2 for c in targets[0]]
    everywhere = count <= 27

    def step(i, total):
        if everywhere:
            upper = coords_of(i, bits)
            q = i
            ok = None
            for a in range(3):
                near = jnp.abs(upper[a] - home[a]) <= 1
                ok = near if ok is None else ok & near
        else:
            upper = [home[0] + i // 9 - 1, home[1] + (i // 3) % 3 - 1, home[2] + i % 3 - 1]
            ok = inside(upper, bits)
            q = jnp.where(ok, index_of([jnp.maximum(u, 0) for u in upper], bits), 0)
        mats = []
        for target in targets:
            column = []
            for h in range(8):
                d = [2 * upper[a] + (h >> a & 1) - target[a] for a in range(3)]
                apart = (jnp.abs(d[0]) > 1) | (jnp.abs(d[1]) > 1) | (jnp.abs(d[2]) > 1)
                use = ok & apart
                code = (SPAN * (d[0] + REACH) + d[1] + REACH) * SPAN + d[2] + REACH
                code = jnp.where(use, code, 0)
                mat = table[pl.ds(code, half, stride=pitch), :]
                mat = mat * jnp.where(use, 1.0, 0.0).astype(F32)
                column.append(mat.astype(BF16))
            mats.append(jnp.concatenate(column, axis=0))
        mats = jnp.concatenate(mats, axis=1) if len(mats) > 1 else mats[0]
        rows = pl.ds(pl.multiple_of(q * 8 * half, 8 * half), 8 * half)
        return total + lax.dot_general(
            stacked[rows, :], mats, TN, preferred_element_type=F32
        )

    start = jnp.zeros((2 * rank, 2 * rank * len(targets)), F32)
    total = lax.fori_loop(0, min(count, 27), step, start)
    result = []
    for l in range(len(targets)):
        part = total[:, 2 * rank * l : 2 * rank * (l + 1)]
        result.append(part[:rank, :rank] + part[rank:, rank:])
    return result


def kernel(
    n,
    panels,
    basis,
    transfer,
    blocks_hbm,
    coupling_hbm,
    near_list,
    out,
    all_panels,
    blocks,
    coupling,
    table0,
    table1,
    coefs,
    parts,
    clusters,
    blocks_sem,
    coupling_sem,
    panel_send,
    panel_recv,
    coef_send,
    coef_recv,
    relay_send,
    relay_recv,
    part_send,
    part_recv,
    cluster_send,
    cluster_recv,
):
    leaf_dev, columns, points = panels.shape
    rank = basis.shape[1]
    slots = near_list.shape[1]
    half = rank // 2
    pitch = table0.shape[0] // half
    shifts = coupling.shape[1]
    low_bits = leaf_dev.bit_length() - 1
    dev_bits = n.bit_length() - 1
    bit_count = low_bits + dev_bits
    group = 8 // leaf_dev
    groups = n // group
    chips = n // 2
    own_rows = leaf_dev * half
    me = lax.axis_index("leaf")
    chip, core = me // 2, me % 2
    mate = chip * 2 + 1 - core

    loads = []
    for level in range(2):
        loads.append(
            pltpu.make_async_copy(
                coupling_hbm.at[level], coupling.at[level], coupling_sem.at[level]
            )
        )
    cut = slots // 3 if slots % 3 == 0 else slots
    for l in range(leaf_dev):
        for i in range(slots // cut):
            rows = pl.ds(i * cut, cut)
            loads.append(
                pltpu.make_async_copy(
                    blocks_hbm.at[l, rows],
                    blocks.at[l, rows],
                    blocks_sem.at[l * (slots // cut) + i],
                )
            )
    for load in loads:
        load.start()

    barrier = pltpu.get_barrier_semaphore()

    @pl.loop(1, n)
    def _(j):
        pl.semaphore_signal(
            barrier, inc=1, device_id=(lax.rem(me + j, n),), device_id_type=MESH
        )

    row = lax.broadcasted_iota(jnp.int32, (rank, rank), 0)
    col = lax.broadcasted_iota(jnp.int32, (rank, rank), 1)
    source = 2 * (row % half) + row // half
    order = jnp.where(col == source, 1.0, 0.0).astype(BF16)
    term = jnp.zeros((rank, columns), F32)
    for l in range(leaf_dev):
        flat = lax.dot_general(
            basis[l], panels[l], NT, preferred_element_type=F32
        ).astype(BF16)
        mixed = jnp.dot(order, flat, preferred_element_type=F32).astype(BF16)
        packed = jnp.concatenate([mixed[:half], mixed[half:]], axis=1)
        at = pl.multiple_of(me * own_rows, own_rows) + l * half
        coefs[pl.ds(pl.multiple_of(at, half), half), :] = packed
        sent = lax.dot_general(
            order, transfer[l], NT, preferred_element_type=F32
        ).astype(BF16)
        term = term + jnp.dot(sent, flat, preferred_element_type=F32)
    parts[0] = jnp.concatenate([term[:half], term[half:]], axis=1)
    for l in range(leaf_dev):
        all_panels[me * leaf_dev + l] = panels[l]

    pl.semaphore_wait(barrier, n - 1)

    def own_block(device):
        return coefs.at[pl.ds(pl.multiple_of(device * own_rows, own_rows), own_rows), :]

    def coef_copy(m, device):
        to = lax.rem(chip + m, chips) * 2 + core
        return pltpu.make_async_remote_copy(
            src_ref=own_block(device),
            dst_ref=own_block(device),
            send_sem=coef_send.at[m],
            recv_sem=coef_recv.at[m],
            device_id=(to,),
            device_id_type=MESH,
        )

    def relay_copy(m, device):
        return pltpu.make_async_remote_copy(
            src_ref=own_block(device),
            dst_ref=own_block(device),
            send_sem=relay_send.at[m],
            recv_sem=relay_recv.at[m],
            device_id=(mate,),
            device_id_type=MESH,
        )

    def part_copy(j):
        base = (me // group) * group
        return pltpu.make_async_remote_copy(
            src_ref=parts.at[0],
            dst_ref=parts.at[j],
            send_sem=part_send.at[j],
            recv_sem=part_recv.at[j],
            device_id=(base + lax.rem(me - base + j, group),),
            device_id_type=MESH,
        )

    def cluster_block(p):
        return clusters.at[pl.ds(pl.multiple_of(p * half, half), half), :]

    def cluster_copy(j, p):
        return pltpu.make_async_remote_copy(
            src_ref=cluster_block(p),
            dst_ref=cluster_block(p),
            send_sem=cluster_send.at[j],
            recv_sem=cluster_recv.at[j],
            device_id=(lax.rem(me + j * group, n),),
            device_id_type=MESH,
        )

    bits = axis_bits(low_bits, dev_bits)
    where = coords_of(me, bits)

    def panel_copy(o, sender, receiver):
        first, count = 0, leaf_dev
        if leaf_dev == 2 and OFFSETS[o][0] != 0:
            first, count = (1 if OFFSETS[o][0] > 0 else 0), 1
        return pltpu.make_async_remote_copy(
            src_ref=panels.at[pl.ds(first, count)],
            dst_ref=all_panels.at[pl.ds(sender * leaf_dev + first, count)],
            send_sem=panel_send.at[o],
            recv_sem=panel_recv.at[o],
            device_id=(receiver,),
            device_id_type=MESH,
        )

    def shifted(o, sign):
        moved = [where[a] + sign * OFFSETS[o][a] for a in range(3)]
        ok = inside(moved, bits)
        return ok, jnp.where(ok, index_of([jnp.maximum(v, 0) for v in moved], bits), 0)

    reach = [o for o in range(27) if OFFSETS[o] != (0, 0, 0)]

    for j in range(1, group):
        part_copy(j).start()
    relay_copy(0, me).start()

    @pl.loop(1, chips)
    def _(m):
        coef_copy(m, me).start()

    for o in reach:
        ok, to = shifted(o, 1)

        @pl.when(ok)
        def _():
            panel_copy(o, me, to).start()

    def unfold(level, table):
        @pl.loop(0, half)
        def _(k):
            lanes = pl.ds(pl.multiple_of(k * 2 * rank, 2 * rank), 2 * rank)
            rows = pl.ds(pl.multiple_of(k * pitch, 8), shifts)
            table[rows, :] = coupling[level, :, lanes].astype(F32)

    for j in range(1, group):
        part_copy(j).wait_recv()
    mine = me // group
    total = parts[0]
    for j in range(1, group):
        total = total + parts[j]
    clusters[pl.ds(pl.multiple_of(mine * half, half), half), :] = total.astype(BF16)
    loads[0].wait()
    unfold(0, table0)

    @pl.loop(1, groups)
    def _(j):
        cluster_copy(j, mine).start()

    @pl.loop(1, chips)
    def _(m):
        coef_copy(m, me).wait_recv()
        relay_copy(m, lax.rem(chip - m + chips, chips) * 2 + core).start()

    loads[1].wait()
    unfold(1, table1)

    @pl.loop(0, chips)
    def _(m):
        relay_copy(m, me).wait_recv()

    leaf_bits = axis_bits(0, bit_count)
    targets = [coords_of(me * leaf_dev + l, leaf_bits) for l in range(leaf_dev)]
    leaf_far = far_sum(targets, bit_count, coefs, table0, pitch, rank)

    @pl.loop(1, groups)
    def _(j):
        cluster_copy(j, mine).wait_recv()

    parent = coords_of(mine, axis_bits(0, bit_count - 3))
    down = far_sum([parent], bit_count - 3, clusters, table1, pitch, rank)[0].astype(BF16)
    far_terms = []
    for l in range(leaf_dev):
        far = leaf_far[l] + lax.dot_general(down, transfer[l], NT, preferred_element_type=F32)
        far_terms.append(jnp.dot(far.astype(BF16), basis[l], preferred_element_type=F32))

    for o in reach:
        ok, sender = shifted(o, -1)

        @pl.when(ok)
        def _():
            panel_copy(o, sender, me).wait_recv()

    for load in loads[2:]:
        load.wait()
    for l in range(leaf_dev):
        total = far_terms[l]
        for k in range(slots):
            j = near_list[l, k]
            block = all_panels[jnp.maximum(j, 0)]
            block = jnp.where(j >= 0, block, jnp.zeros_like(block))
            total = total + jnp.dot(block, blocks[l, k], preferred_element_type=F32)
        out[l] = total.astype(BF16)

    for j in range(1, group):
        part_copy(j).wait_send()

    @pl.loop(0, chips)
    def _(m):
        relay_copy(m, me).wait_send()

    @pl.loop(1, chips)
    def _(m):
        coef_copy(m, me).wait_send()

    @pl.loop(1, groups)
    def _(j):
        cluster_copy(j, mine).wait_send()

    for o in reach:
        ok, to = shifted(o, 1)

        @pl.when(ok)
        def _():
            panel_copy(o, me, to).wait_send()


def per_device(panels, basis, transfer, near_blocks, coupling, near_list):
    n = lax.axis_size("leaf")
    leaf_dev, columns, points = panels.shape
    rank = basis.shape[1]
    slots = near_list.shape[1]
    shifts = coupling.shape[1]
    half = rank // 2
    pitch = -(-shifts // 8) * 8
    leaves = n * leaf_dev
    group = 8 // leaf_dev
    vmem = pl.BlockSpec(memory_space=pltpu.VMEM)
    hbm = pl.BlockSpec(memory_space=pl.ANY)
    dma = pltpu.SemaphoreType.DMA
    return pl.pallas_call(
        functools.partial(kernel, n),
        out_shape=jax.ShapeDtypeStruct(panels.shape, BF16),
        in_specs=[vmem, vmem, vmem, hbm, hbm, pl.BlockSpec(memory_space=pltpu.SMEM)],
        out_specs=vmem,
        scratch_shapes=[
            pltpu.VMEM((leaves, columns, points), BF16),
            pltpu.VMEM(near_blocks.shape, BF16),
            pltpu.VMEM(coupling.shape, BF16),
            pltpu.VMEM((half * pitch, 2 * rank), F32),
            pltpu.VMEM((half * pitch, 2 * rank), F32),
            pltpu.VMEM((leaves * half, 2 * columns), BF16),
            pltpu.VMEM((group, half, 2 * columns), F32),
            pltpu.VMEM((n // group * half, 2 * columns), BF16),
            dma((leaf_dev * 3,)),
            dma((2,)),
            dma((27,)),
            dma((27,)),
            dma((n // 2,)),
            dma((n // 2,)),
            dma((n // 2,)),
            dma((n // 2,)),
            dma((group,)),
            dma((group,)),
            dma((n // group,)),
            dma((n // group,)),
        ],
        compiler_params=pltpu.CompilerParams(
            collective_id=0, has_side_effects=True, vmem_limit_bytes=60 * 2**20
        ),
    )(panels, basis, transfer, near_blocks, coupling, near_list)


def solution(mesh):
    placed = (
        P("leaf", None, None),
        P("leaf", None, None),
        P("leaf", None, None),
        P("leaf", None, None, None),
        P(),
        P("leaf", None),
    )
    return jax.shard_map(
        per_device, mesh=mesh, in_specs=placed, out_specs=P("leaf", None, None), check_vma=False
    )
```

```python
import functools

import jax
import jax.numpy as jnp
from jax import lax
from jax.experimental import pallas as pl
from jax.experimental.pallas import tpu as pltpu
from jax.sharding import PartitionSpec as P

MESH = pl.DeviceIdType.MESH
F32 = jnp.float32
BF16 = jnp.bfloat16
REACH = 3
SPAN = 2 * REACH + 1
TN = (((0,), (0,)), ((), ()))
NT = (((1,), (1,)), ((), ()))
OFFSETS = [(a, b, c) for a in (-1, 0, 1) for b in (-1, 0, 1) for c in (-1, 0, 1)]


def axis_bits(first, bit_count):
    return [[b for b in range(bit_count) if (b + first) % 3 == a] for a in range(3)]


def coords_of(index, bits):
    return [
        sum(((index // 2**b) % 2) * 2**p for p, b in enumerate(bits[a])) + index * 0
        for a in range(3)
    ]


def index_of(coords, bits):
    return sum(((coords[a] // 2**p) % 2) * 2**b for a in range(3) for p, b in enumerate(bits[a]))


def inside(coords, bits):
    ok = None
    for a in range(3):
        here = (coords[a] >= 0) & (coords[a] < 2 ** len(bits[a]))
        ok = here if ok is None else ok & here
    return ok


def far_mats(targets, bit_count, coupling, level, spread, mats):
    half = coupling.shape[1] // 2
    count = 2 ** (bit_count - 3)

    @pl.loop(0, min(count, 27))
    def _(i):
        upper, _, ok = candidate(targets[0], bit_count, i)
        columns = []
        for l, target in enumerate(targets):
            column = []
            for h in range(8):
                d = [2 * upper[a] + (h >> a & 1) - target[a] for a in range(3)]
                apart = (jnp.abs(d[0]) > 1) | (jnp.abs(d[1]) > 1) | (jnp.abs(d[2]) > 1)
                use = ok & apart
                code = (SPAN * (d[0] + REACH) + d[1] + REACH) * SPAN + d[2] + REACH
                code = jnp.where(use, code, 0)
                at = (l * 8 + h) * 2 * half
                spread[at : at + 2 * half, :] = coupling[code].astype(F32)
                mat = spread[pl.ds(at + level, half, stride=2), :]
                mat = mat * jnp.where(use, 1.0, 0.0).astype(F32)
                column.append(mat.astype(BF16))
            columns.append(jnp.concatenate(column, axis=0))
        mats[i] = jnp.concatenate(columns, axis=1) if len(columns) > 1 else columns[0]


def candidate(target, bit_count, i):
    bits = axis_bits(0, bit_count - 3)
    home = [c // 2 for c in target]
    if 2 ** (bit_count - 3) <= 27:
        upper = coords_of(i, bits)
        ok = None
        for a in range(3):
            near = jnp.abs(upper[a] - home[a]) <= 1
            ok = near if ok is None else ok & near
        return upper, i, ok
    upper = [home[0] + i // 9 - 1, home[1] + (i // 3) % 3 - 1, home[2] + i % 3 - 1]
    ok = inside(upper, bits)
    return upper, jnp.where(ok, index_of([jnp.maximum(u, 0) for u in upper], bits), 0), ok


def far_sum(targets, bit_count, stacked, mats, rank):
    depth = 8 * rank // 2
    count = 2 ** (bit_count - 3)

    def step(i, total):
        _, q, _ = candidate(targets[0], bit_count, i)
        rows = pl.ds(pl.multiple_of(q * depth, depth), depth)
        return total + lax.dot_general(stacked[rows, :], mats[i], TN, preferred_element_type=F32)

    start = jnp.zeros((2 * rank, 2 * rank * len(targets)), F32)
    total = lax.fori_loop(0, min(count, 27), step, start)
    result = []
    for l in range(len(targets)):
        part = total[:, 2 * rank * l : 2 * rank * (l + 1)]
        result.append(part[:rank, :rank] + part[rank:, rank:])
    return result


def kernel(
    n,
    panels,
    basis,
    transfer,
    blocks_hbm,
    coupling_hbm,
    near_list,
    out,
    all_panels,
    blocks,
    coupling,
    spread,
    mats0,
    mats1,
    coefs,
    parts,
    clusters,
    blocks_sem,
    coupling_sem,
    panel_send,
    panel_recv,
    coef_send,
    coef_recv,
    relay_send,
    relay_recv,
    part_send,
    part_recv,
    cluster_send,
    cluster_recv,
):
    leaf_dev, columns, points = panels.shape
    rank = basis.shape[1]
    slots = near_list.shape[1]
    half = rank // 2
    low_bits = leaf_dev.bit_length() - 1
    dev_bits = n.bit_length() - 1
    bit_count = low_bits + dev_bits
    group = 8 // leaf_dev
    groups = n // group
    chips = n // 2
    own_rows = leaf_dev * half
    me = lax.axis_index("leaf")
    chip, core = me // 2, me % 2
    mate = chip * 2 + 1 - core

    loads = [pltpu.make_async_copy(coupling_hbm, coupling, coupling_sem)]
    cut = slots // 3 if slots % 3 == 0 else slots
    for l in range(leaf_dev):
        for i in range(slots // cut):
            rows = pl.ds(i * cut, cut)
            loads.append(
                pltpu.make_async_copy(
                    blocks_hbm.at[l, rows],
                    blocks.at[l, rows],
                    blocks_sem.at[l * (slots // cut) + i],
                )
            )
    for load in loads:
        load.start()

    barrier = pltpu.get_barrier_semaphore()

    @pl.loop(1, n)
    def _(j):
        pl.semaphore_signal(
            barrier, inc=1, device_id=(lax.rem(me + j, n),), device_id_type=MESH
        )

    row = lax.broadcasted_iota(jnp.int32, (rank, rank), 0)
    col = lax.broadcasted_iota(jnp.int32, (rank, rank), 1)
    source = 2 * (row % half) + row // half
    order = jnp.where(col == source, 1.0, 0.0).astype(BF16)
    term = jnp.zeros((rank, columns), F32)
    for l in range(leaf_dev):
        flat = lax.dot_general(
            basis[l], panels[l], NT, preferred_element_type=F32
        ).astype(BF16)
        mixed = jnp.dot(order, flat, preferred_element_type=F32).astype(BF16)
        packed = jnp.concatenate([mixed[:half], mixed[half:]], axis=1)
        at = pl.multiple_of(me * own_rows, own_rows) + l * half
        coefs[pl.ds(pl.multiple_of(at, half), half), :] = packed
        sent = lax.dot_general(
            order, transfer[l], NT, preferred_element_type=F32
        ).astype(BF16)
        term = term + jnp.dot(sent, flat, preferred_element_type=F32)
    parts[0] = jnp.concatenate([term[:half], term[half:]], axis=1)
    for l in range(leaf_dev):
        all_panels[me * leaf_dev + l] = panels[l]

    pl.semaphore_wait(barrier, n - 1)

    def own_block(device):
        return coefs.at[pl.ds(pl.multiple_of(device * own_rows, own_rows), own_rows), :]

    def coef_copy(m, device):
        to = lax.rem(chip + m, chips) * 2 + core
        return pltpu.make_async_remote_copy(
            src_ref=own_block(device),
            dst_ref=own_block(device),
            send_sem=coef_send.at[m],
            recv_sem=coef_recv.at[m],
            device_id=(to,),
            device_id_type=MESH,
        )

    def relay_copy(m, device):
        return pltpu.make_async_remote_copy(
            src_ref=own_block(device),
            dst_ref=own_block(device),
            send_sem=relay_send.at[m],
            recv_sem=relay_recv.at[m],
            device_id=(mate,),
            device_id_type=MESH,
        )

    def part_copy(j):
        base = (me // group) * group
        return pltpu.make_async_remote_copy(
            src_ref=parts.at[0],
            dst_ref=parts.at[j],
            send_sem=part_send.at[j],
            recv_sem=part_recv.at[j],
            device_id=(base + lax.rem(me - base + j, group),),
            device_id_type=MESH,
        )

    def cluster_block(p):
        return clusters.at[pl.ds(pl.multiple_of(p * half, half), half), :]

    def cluster_copy(j, p):
        return pltpu.make_async_remote_copy(
            src_ref=cluster_block(p),
            dst_ref=cluster_block(p),
            send_sem=cluster_send.at[j],
            recv_sem=cluster_recv.at[j],
            device_id=(lax.rem(me + j * group, n),),
            device_id_type=MESH,
        )

    bits = axis_bits(low_bits, dev_bits)
    where = coords_of(me, bits)

    def panel_copy(o, sender, receiver):
        first, count = 0, leaf_dev
        if leaf_dev == 2 and OFFSETS[o][0] != 0:
            first, count = (1 if OFFSETS[o][0] > 0 else 0), 1
        return pltpu.make_async_remote_copy(
            src_ref=panels.at[pl.ds(first, count)],
            dst_ref=all_panels.at[pl.ds(sender * leaf_dev + first, count)],
            send_sem=panel_send.at[o],
            recv_sem=panel_recv.at[o],
            device_id=(receiver,),
            device_id_type=MESH,
        )

    def shifted(o, sign):
        moved = [where[a] + sign * OFFSETS[o][a] for a in range(3)]
        ok = inside(moved, bits)
        return ok, jnp.where(ok, index_of([jnp.maximum(v, 0) for v in moved], bits), 0)

    reach = [o for o in range(27) if OFFSETS[o] != (0, 0, 0)]

    for j in range(1, group):
        part_copy(j).start()
    relay_copy(0, me).start()

    @pl.loop(1, chips)
    def _(m):
        coef_copy(m, me).start()

    for o in reach:
        ok, to = shifted(o, 1)

        @pl.when(ok)
        def _():
            panel_copy(o, me, to).start()

    for j in range(1, group):
        part_copy(j).wait_recv()
    mine = me // group
    total = parts[0]
    for j in range(1, group):
        total = total + parts[j]
    clusters[pl.ds(pl.multiple_of(mine * half, half), half), :] = total.astype(BF16)
    parent = coords_of(mine, axis_bits(0, bit_count - 3))
    loads[0].wait()
    far_mats([parent], bit_count - 3, coupling, 1, spread, mats1)

    @pl.loop(1, groups)
    def _(j):
        cluster_copy(j, mine).start()

    @pl.loop(1, chips)
    def _(m):
        coef_copy(m, me).wait_recv()
        relay_copy(m, lax.rem(chip - m + chips, chips) * 2 + core).start()

    leaf_bits = axis_bits(0, bit_count)
    targets = [coords_of(me * leaf_dev + l, leaf_bits) for l in range(leaf_dev)]
    far_mats(targets, bit_count, coupling, 0, spread, mats0)

    @pl.loop(0, chips)
    def _(m):
        relay_copy(m, me).wait_recv()

    leaf_far = far_sum(targets, bit_count, coefs, mats0, rank)

    @pl.loop(1, groups)
    def _(j):
        cluster_copy(j, mine).wait_recv()

    down = far_sum([parent], bit_count - 3, clusters, mats1, rank)[0].astype(BF16)
    far_terms = []
    for l in range(leaf_dev):
        far = leaf_far[l] + lax.dot_general(down, transfer[l], NT, preferred_element_type=F32)
        far_terms.append(jnp.dot(far.astype(BF16), basis[l], preferred_element_type=F32))

    for o in reach:
        ok, sender = shifted(o, -1)

        @pl.when(ok)
        def _():
            panel_copy(o, sender, me).wait_recv()

    for load in loads[1:]:
        load.wait()
    for l in range(leaf_dev):
        total = far_terms[l]
        for k in range(slots):
            j = near_list[l, k]
            block = all_panels[jnp.maximum(j, 0)]
            block = jnp.where(j >= 0, block, jnp.zeros_like(block))
            total = total + jnp.dot(block, blocks[l, k], preferred_element_type=F32)
        out[l] = total.astype(BF16)

    for j in range(1, group):
        part_copy(j).wait_send()

    @pl.loop(0, chips)
    def _(m):
        relay_copy(m, me).wait_send()

    @pl.loop(1, chips)
    def _(m):
        coef_copy(m, me).wait_send()

    @pl.loop(1, groups)
    def _(j):
        cluster_copy(j, mine).wait_send()

    for o in reach:
        ok, to = shifted(o, 1)

        @pl.when(ok)
        def _():
            panel_copy(o, me, to).wait_send()


def per_device(panels, basis, transfer, near_blocks, coupling, near_list):
    n = lax.axis_size("leaf")
    leaf_dev, columns, points = panels.shape
    rank = basis.shape[1]
    slots = near_list.shape[1]
    shifts = coupling.shape[1]
    half = rank // 2
    leaves = n * leaf_dev
    coupling = coupling.transpose(1, 0, 2).reshape(shifts, 2, half, 2 * rank)
    coupling = coupling.transpose(0, 2, 1, 3).reshape(shifts, rank, 2 * rank)
    group = 8 // leaf_dev
    vmem = pl.BlockSpec(memory_space=pltpu.VMEM)
    hbm = pl.BlockSpec(memory_space=pl.ANY)
    dma = pltpu.SemaphoreType.DMA
    return pl.pallas_call(
        functools.partial(kernel, n),
        out_shape=jax.ShapeDtypeStruct(panels.shape, BF16),
        in_specs=[vmem, vmem, vmem, hbm, hbm, pl.BlockSpec(memory_space=pltpu.SMEM)],
        out_specs=vmem,
        scratch_shapes=[
            pltpu.VMEM((leaves, columns, points), BF16),
            pltpu.VMEM(near_blocks.shape, BF16),
            pltpu.VMEM(coupling.shape, BF16),
            pltpu.VMEM((leaf_dev * 8 * rank, 2 * rank), F32),
            pltpu.VMEM((min(leaves // 8, 27), 8 * half, 2 * rank * leaf_dev), BF16),
            pltpu.VMEM((min(leaves // 64, 27), 8 * half, 2 * rank), BF16),
            pltpu.VMEM((leaves * half, 2 * columns), BF16),
            pltpu.VMEM((group, half, 2 * columns), F32),
            pltpu.VMEM((n // group * half, 2 * columns), BF16),
            dma((leaf_dev * 3,)),
            dma,
            dma((27,)),
            dma((27,)),
            dma((n // 2,)),
            dma((n // 2,)),
            dma((n // 2,)),
            dma((n // 2,)),
            dma((group,)),
            dma((group,)),
            dma((n // group,)),
            dma((n // group,)),
        ],
        compiler_params=pltpu.CompilerParams(
            collective_id=0, has_side_effects=True, vmem_limit_bytes=60 * 2**20
        ),
    )(panels, basis, transfer, near_blocks, coupling, near_list)


def solution(mesh):
    placed = (
        P("leaf", None, None),
        P("leaf", None, None),
        P("leaf", None, None),
        P("leaf", None, None, None),
        P(),
        P("leaf", None),
    )
    return jax.shard_map(
        per_device, mesh=mesh, in_specs=placed, out_specs=P("leaf", None, None), check_vma=False
    )
```

```python
import functools

import jax
import jax.numpy as jnp
from jax import lax
from jax.experimental import pallas as pl
from jax.experimental.pallas import tpu as pltpu
from jax.sharding import PartitionSpec as P

MESH = pl.DeviceIdType.MESH
F32 = jnp.float32
BF16 = jnp.bfloat16
REACH = 3
SPAN = 2 * REACH + 1
TN = (((0,), (0,)), ((), ()))
NT = (((1,), (1,)), ((), ()))
OFFSETS = [(a, b, c) for a in (-1, 0, 1) for b in (-1, 0, 1) for c in (-1, 0, 1)]


def axis_bits(first, bit_count):
    return [[b for b in range(bit_count) if (b + first) % 3 == a] for a in range(3)]


def coords_of(index, bits):
    return [
        sum(((index // 2**b) % 2) * 2**p for p, b in enumerate(bits[a])) + index * 0
        for a in range(3)
    ]


def index_of(coords, bits):
    return sum(((coords[a] // 2**p) % 2) * 2**b for a in range(3) for p, b in enumerate(bits[a]))


def inside(coords, bits):
    ok = None
    for a in range(3):
        here = (coords[a] >= 0) & (coords[a] < 2 ** len(bits[a]))
        ok = here if ok is None else ok & here
    return ok


def far_mats(targets, bit_count, coupling, level, spread, mats):
    half = coupling.shape[1] // 2
    count = 2 ** (bit_count - 3)

    @pl.loop(0, min(count, 27))
    def _(i):
        upper, _, ok = candidate(targets[0], bit_count, i)
        columns = []
        for l, target in enumerate(targets):
            column = []
            for h in range(8):
                d = [2 * upper[a] + (h >> a & 1) - target[a] for a in range(3)]
                apart = (jnp.abs(d[0]) > 1) | (jnp.abs(d[1]) > 1) | (jnp.abs(d[2]) > 1)
                use = ok & apart
                code = (SPAN * (d[0] + REACH) + d[1] + REACH) * SPAN + d[2] + REACH
                code = jnp.where(use, code, 0)
                at = (l * 8 + h) * 2 * half
                spread[at : at + 2 * half, :] = coupling[code].astype(F32)
                mat = spread[pl.ds(at + level, half, stride=2), :]
                mat = mat * jnp.where(use, 1.0, 0.0).astype(F32)
                column.append(mat.astype(BF16))
            columns.append(jnp.concatenate(column, axis=0))
        mats[i] = jnp.concatenate(columns, axis=1) if len(columns) > 1 else columns[0]


def candidate(target, bit_count, i):
    bits = axis_bits(0, bit_count - 3)
    home = [c // 2 for c in target]
    if 2 ** (bit_count - 3) <= 27:
        upper = coords_of(i, bits)
        ok = None
        for a in range(3):
            near = jnp.abs(upper[a] - home[a]) <= 1
            ok = near if ok is None else ok & near
        return upper, i, ok
    upper = [home[0] + i // 9 - 1, home[1] + (i // 3) % 3 - 1, home[2] + i % 3 - 1]
    ok = inside(upper, bits)
    return upper, jnp.where(ok, index_of([jnp.maximum(u, 0) for u in upper], bits), 0), ok


def far_sum(targets, bit_count, stacked, mats, rank):
    depth = 8 * rank // 2
    count = 2 ** (bit_count - 3)

    def step(i, total):
        _, q, _ = candidate(targets[0], bit_count, i)
        rows = pl.ds(pl.multiple_of(q * depth, depth), depth)
        return total + lax.dot_general(stacked[rows, :], mats[i], TN, preferred_element_type=F32)

    start = jnp.zeros((2 * rank, 2 * rank * len(targets)), F32)
    total = lax.fori_loop(0, min(count, 27), step, start)
    result = []
    for l in range(len(targets)):
        part = total[:, 2 * rank * l : 2 * rank * (l + 1)]
        result.append(part[:rank, :rank] + part[rank:, rank:])
    return result


def kernel(
    n,
    panels,
    basis,
    transfer,
    blocks_hbm,
    coupling_hbm,
    near_list,
    out,
    all_panels,
    blocks,
    coupling,
    spread,
    mats0,
    mats1,
    coefs,
    parts,
    clusters,
    blocks_sem,
    coupling_sem,
    panel_send,
    panel_recv,
    coef_send,
    coef_recv,
    relay_send,
    relay_recv,
    part_send,
    part_recv,
    cluster_send,
    cluster_recv,
):
    leaf_dev, columns, points = panels.shape
    rank = basis.shape[1]
    slots = near_list.shape[1]
    half = rank // 2
    low_bits = leaf_dev.bit_length() - 1
    dev_bits = n.bit_length() - 1
    bit_count = low_bits + dev_bits
    group = 8 // leaf_dev
    groups = n // group
    chips = n // 2
    own_rows = leaf_dev * half
    me = lax.axis_index("leaf")
    chip, core = me // 2, me % 2
    mate = chip * 2 + 1 - core

    loads = [pltpu.make_async_copy(coupling_hbm, coupling, coupling_sem)]
    cut = slots // 3 if slots % 3 == 0 else slots
    for l in range(leaf_dev):
        for i in range(slots // cut):
            rows = pl.ds(i * cut, cut)
            loads.append(
                pltpu.make_async_copy(
                    blocks_hbm.at[l, rows],
                    blocks.at[l, rows],
                    blocks_sem.at[l * (slots // cut) + i],
                )
            )
    for load in loads:
        load.start()

    barrier = pltpu.get_barrier_semaphore()

    @pl.loop(1, n)
    def _(j):
        pl.semaphore_signal(
            barrier, inc=1, device_id=(lax.rem(me + j, n),), device_id_type=MESH
        )

    row = lax.broadcasted_iota(jnp.int32, (rank, rank), 0)
    col = lax.broadcasted_iota(jnp.int32, (rank, rank), 1)
    source = 2 * (row % half) + row // half
    order = jnp.where(col == source, 1.0, 0.0).astype(BF16)
    term = jnp.zeros((rank, columns), F32)
    for l in range(leaf_dev):
        flat = lax.dot_general(
            basis[l], panels[l], NT, preferred_element_type=F32
        ).astype(BF16)
        mixed = jnp.dot(order, flat, preferred_element_type=F32).astype(BF16)
        packed = jnp.concatenate([mixed[:half], mixed[half:]], axis=1)
        at = pl.multiple_of(me * own_rows, own_rows) + l * half
        coefs[pl.ds(pl.multiple_of(at, half), half), :] = packed
        sent = lax.dot_general(
            order, transfer[l], NT, preferred_element_type=F32
        ).astype(BF16)
        term = term + jnp.dot(sent, flat, preferred_element_type=F32)
    parts[0] = jnp.concatenate([term[:half], term[half:]], axis=1)
    for l in range(leaf_dev):
        all_panels[me * leaf_dev + l] = panels[l]

    pl.semaphore_wait(barrier, n - 1)

    def own_block(device):
        return coefs.at[pl.ds(pl.multiple_of(device * own_rows, own_rows), own_rows), :]

    places = min(4, chips)
    columns_of_chips = chips // places
    line, place = chip // places, lax.rem(chip, places)

    def coef_device(j, k):
        from_line = lax.rem(line - j + columns_of_chips, columns_of_chips)
        from_place = lax.rem(place - k + places, places)
        return (from_line * places + from_place) * 2 + core

    def coef_copy(j, k):
        to_line = lax.rem(line + j, columns_of_chips) if k is None else line
        to_place = place if k is None else lax.rem(place + k, places)
        m = j * places + (0 if k is None else k)
        block = own_block(me) if k is None else own_block(coef_device(j, 0))
        return pltpu.make_async_remote_copy(
            src_ref=block,
            dst_ref=block,
            send_sem=coef_send.at[m],
            recv_sem=coef_recv.at[m],
            device_id=((to_line * places + to_place) * 2 + core,),
            device_id_type=MESH,
        )

    def relay_copy(m, device):
        return pltpu.make_async_remote_copy(
            src_ref=own_block(device),
            dst_ref=own_block(device),
            send_sem=relay_send.at[m],
            recv_sem=relay_recv.at[m],
            device_id=(mate,),
            device_id_type=MESH,
        )

    def part_copy(j):
        base = (me // group) * group
        return pltpu.make_async_remote_copy(
            src_ref=parts.at[0],
            dst_ref=parts.at[j],
            send_sem=part_send.at[j],
            recv_sem=part_recv.at[j],
            device_id=(base + lax.rem(me - base + j, group),),
            device_id_type=MESH,
        )

    def cluster_block(p):
        return clusters.at[pl.ds(pl.multiple_of(p * half, half), half), :]

    def cluster_copy(j, p):
        return pltpu.make_async_remote_copy(
            src_ref=cluster_block(p),
            dst_ref=cluster_block(p),
            send_sem=cluster_send.at[j],
            recv_sem=cluster_recv.at[j],
            device_id=(lax.rem(me + j * group, n),),
            device_id_type=MESH,
        )

    bits = axis_bits(low_bits, dev_bits)
    where = coords_of(me, bits)

    def hop_of(o):
        x, y, z = OFFSETS[o]
        return (0, y, 0) if y else (x, 0, 0) if x else (0, 0, z)

    def moved(offset):
        there = [where[a] + offset[a] for a in range(3)]
        ok = inside(there, bits)
        return ok, jnp.where(ok, index_of([jnp.maximum(v, 0) for v in there], bits), 0)

    def panel_copy(o, source, receiver):
        first, count = 0, leaf_dev
        if leaf_dev == 2 and OFFSETS[o][0] != 0:
            first, count = (1 if OFFSETS[o][0] > 0 else 0), 1
        rows = pl.ds(source * leaf_dev + first, count)
        owned = hop_of(o) == OFFSETS[o]
        return pltpu.make_async_remote_copy(
            src_ref=panels.at[pl.ds(first, count)] if owned else all_panels.at[rows],
            dst_ref=all_panels.at[rows],
            send_sem=panel_send.at[o],
            recv_sem=panel_recv.at[o],
            device_id=(receiver,),
            device_id_type=MESH,
        )

    def sends(o, act):
        hop = hop_of(o)
        ok, to = moved(hop)
        known, source = moved([h - e for h, e in zip(hop, OFFSETS[o])])

        @pl.when(ok & known)
        def _():
            act(panel_copy(o, source, to))

    def receives(o):
        known, source = moved([-e for e in OFFSETS[o]])

        @pl.when(known)
        def _():
            panel_copy(o, source, me).wait_recv()

    reach = [o for o in range(27) if OFFSETS[o] != (0, 0, 0)]
    along_z = [o for o in reach if not OFFSETS[o][0] and not OFFSETS[o][1]]
    along_x = [o for o in reach if OFFSETS[o][0] and not OFFSETS[o][1]]
    along_y = [o for o in reach if OFFSETS[o][1]]

    def start(copy):
        copy.start()

    for j in range(1, group):
        part_copy(j).start()
    for o in along_z:
        sends(o, start)

    @pl.loop(1, columns_of_chips)
    def _(j):
        coef_copy(j, None).start()

    relay_copy(0, me).start()
    for k in range(1, places):
        coef_copy(0, k).start()
    for o in along_x + along_y:
        if hop_of(o) == OFFSETS[o]:
            sends(o, start)

    for j in range(1, group):
        part_copy(j).wait_recv()
    mine = me // group
    total = parts[0]
    for j in range(1, group):
        total = total + parts[j]
    clusters[pl.ds(pl.multiple_of(mine * half, half), half), :] = total.astype(BF16)

    for o in along_z:
        receives(o)
        for later in along_x + along_y:
            before = [e - h for e, h in zip(OFFSETS[later], hop_of(later))]
            if tuple(before) == OFFSETS[o]:
                sends(later, start)

    @pl.loop(1, columns_of_chips)
    def _(j):
        coef_copy(j, None).wait_recv()
        for k in range(1, places):
            coef_copy(j, k).start()
        relay_copy(j * places, coef_device(j, 0)).start()

    @pl.loop(1, groups)
    def _(j):
        cluster_copy(j, mine).start()

    for o in along_x:
        receives(o)
        for later in along_y:
            before = [e - h for e, h in zip(OFFSETS[later], hop_of(later))]
            if tuple(before) == OFFSETS[o]:
                sends(later, start)

    @pl.loop(0, columns_of_chips)
    def _(j):
        for k in range(1, places):
            coef_copy(j, k).wait_recv()
            relay_copy(j * places + k, coef_device(j, k)).start()

    parent = coords_of(mine, axis_bits(0, bit_count - 3))
    leaf_bits = axis_bits(0, bit_count)
    targets = [coords_of(me * leaf_dev + l, leaf_bits) for l in range(leaf_dev)]
    loads[0].wait()
    far_mats([parent], bit_count - 3, coupling, 1, spread, mats1)
    far_mats(targets, bit_count, coupling, 0, spread, mats0)

    @pl.loop(0, chips)
    def _(m):
        relay_copy(m, me).wait_recv()

    leaf_far = far_sum(targets, bit_count, coefs, mats0, rank)

    @pl.loop(1, groups)
    def _(j):
        cluster_copy(j, mine).wait_recv()

    down = far_sum([parent], bit_count - 3, clusters, mats1, rank)[0].astype(BF16)
    far_terms = []
    for l in range(leaf_dev):
        far = leaf_far[l] + lax.dot_general(down, transfer[l], NT, preferred_element_type=F32)
        far_terms.append(jnp.dot(far.astype(BF16), basis[l], preferred_element_type=F32))

    for o in along_y:
        receives(o)
    for load in loads[1:]:
        load.wait()
    for l in range(leaf_dev):
        total = far_terms[l]
        for k in range(slots):
            j = near_list[l, k]
            block = all_panels[jnp.maximum(j, 0)]
            block = jnp.where(j >= 0, block, jnp.zeros_like(block))
            total = total + jnp.dot(block, blocks[l, k], preferred_element_type=F32)
        out[l] = total.astype(BF16)

    for j in range(1, group):
        part_copy(j).wait_send()

    @pl.loop(0, chips)
    def _(m):
        relay_copy(m, me).wait_send()

    @pl.loop(1, columns_of_chips)
    def _(j):
        coef_copy(j, None).wait_send()

    @pl.loop(0, columns_of_chips)
    def _(j):
        for k in range(1, places):
            coef_copy(j, k).wait_send()

    @pl.loop(1, groups)
    def _(j):
        cluster_copy(j, mine).wait_send()

    for o in reach:
        sends(o, lambda copy: copy.wait_send())


def per_device(panels, basis, transfer, near_blocks, coupling, near_list):
    n = lax.axis_size("leaf")
    leaf_dev, columns, points = panels.shape
    rank = basis.shape[1]
    slots = near_list.shape[1]
    shifts = coupling.shape[1]
    half = rank // 2
    leaves = n * leaf_dev
    coupling = coupling.transpose(1, 0, 2).reshape(shifts, 2, half, 2 * rank)
    coupling = coupling.transpose(0, 2, 1, 3).reshape(shifts, rank, 2 * rank)
    group = 8 // leaf_dev
    vmem = pl.BlockSpec(memory_space=pltpu.VMEM)
    hbm = pl.BlockSpec(memory_space=pl.ANY)
    dma = pltpu.SemaphoreType.DMA
    return pl.pallas_call(
        functools.partial(kernel, n),
        out_shape=jax.ShapeDtypeStruct(panels.shape, BF16),
        in_specs=[vmem, vmem, vmem, hbm, hbm, pl.BlockSpec(memory_space=pltpu.SMEM)],
        out_specs=vmem,
        scratch_shapes=[
            pltpu.VMEM((leaves, columns, points), BF16),
            pltpu.VMEM(near_blocks.shape, BF16),
            pltpu.VMEM(coupling.shape, BF16),
            pltpu.VMEM((leaf_dev * 8 * rank, 2 * rank), F32),
            pltpu.VMEM((min(leaves // 8, 27), 8 * half, 2 * rank * leaf_dev), BF16),
            pltpu.VMEM((min(leaves // 64, 27), 8 * half, 2 * rank), BF16),
            pltpu.VMEM((leaves * half, 2 * columns), BF16),
            pltpu.VMEM((group, half, 2 * columns), F32),
            pltpu.VMEM((n // group * half, 2 * columns), BF16),
            dma((leaf_dev * 3,)),
            dma,
            dma((27,)),
            dma((27,)),
            dma((n // 2,)),
            dma((n // 2,)),
            dma((n // 2,)),
            dma((n // 2,)),
            dma((group,)),
            dma((group,)),
            dma((n // group,)),
            dma((n // group,)),
        ],
        compiler_params=pltpu.CompilerParams(
            collective_id=0, has_side_effects=True, vmem_limit_bytes=60 * 2**20
        ),
    )(panels, basis, transfer, near_blocks, coupling, near_list)


def solution(mesh):
    placed = (
        P("leaf", None, None),
        P("leaf", None, None),
        P("leaf", None, None),
        P("leaf", None, None, None),
        P(),
        P("leaf", None),
    )
    return jax.shard_map(
        per_device, mesh=mesh, in_specs=placed, out_specs=P("leaf", None, None), check_vma=False
    )
```

```python
import functools

import jax
import jax.numpy as jnp
from jax import lax
from jax.experimental import pallas as pl
from jax.experimental.pallas import tpu as pltpu
from jax.sharding import PartitionSpec as P

MESH = pl.DeviceIdType.MESH
F32 = jnp.float32
BF16 = jnp.bfloat16
REACH = 3
SPAN = 2 * REACH + 1
TN = (((0,), (0,)), ((), ()))
NT = (((1,), (1,)), ((), ()))
OFFSETS = [(a, b, c) for a in (-1, 0, 1) for b in (-1, 0, 1) for c in (-1, 0, 1)]


def axis_bits(first, bit_count):
    return [[b for b in range(bit_count) if (b + first) % 3 == a] for a in range(3)]


def coords_of(index, bits):
    return [
        sum(((index // 2**b) % 2) * 2**p for p, b in enumerate(bits[a])) + index * 0
        for a in range(3)
    ]


def index_of(coords, bits):
    return sum(((coords[a] // 2**p) % 2) * 2**b for a in range(3) for p, b in enumerate(bits[a]))


def inside(coords, bits):
    ok = None
    for a in range(3):
        here = (coords[a] >= 0) & (coords[a] < 2 ** len(bits[a]))
        ok = here if ok is None else ok & here
    return ok


def far_mats(targets, bit_count, coupling, level, spread, mats):
    half = coupling.shape[1] // 2
    count = 2 ** (bit_count - 3)

    @pl.loop(0, min(count, 27))
    def _(i):
        upper, _, ok = candidate(targets[0], bit_count, i)
        columns = []
        for l, target in enumerate(targets):
            column = []
            for h in range(8):
                d = [2 * upper[a] + (h >> a & 1) - target[a] for a in range(3)]
                apart = (jnp.abs(d[0]) > 1) | (jnp.abs(d[1]) > 1) | (jnp.abs(d[2]) > 1)
                use = ok & apart
                code = (SPAN * (d[0] + REACH) + d[1] + REACH) * SPAN + d[2] + REACH
                code = jnp.where(use, code, 0)
                at = (l * 8 + h) * 2 * half
                spread[at : at + 2 * half, :] = coupling[code].astype(F32)
                mat = spread[pl.ds(at + level, half, stride=2), :]
                mat = mat * jnp.where(use, 1.0, 0.0).astype(F32)
                column.append(mat.astype(BF16))
            columns.append(jnp.concatenate(column, axis=0))
        mats[i] = jnp.concatenate(columns, axis=1) if len(columns) > 1 else columns[0]


def candidate(target, bit_count, i):
    bits = axis_bits(0, bit_count - 3)
    home = [c // 2 for c in target]
    if 2 ** (bit_count - 3) <= 27:
        upper = coords_of(i, bits)
        ok = None
        for a in range(3):
            near = jnp.abs(upper[a] - home[a]) <= 1
            ok = near if ok is None else ok & near
        return upper, i, ok
    upper = [home[0] + i // 9 - 1, home[1] + (i // 3) % 3 - 1, home[2] + i % 3 - 1]
    ok = inside(upper, bits)
    return upper, jnp.where(ok, index_of([jnp.maximum(u, 0) for u in upper], bits), 0), ok


def far_sum(targets, bit_count, stacked, mats, rank):
    depth = 8 * rank // 2
    count = 2 ** (bit_count - 3)

    def step(i, total):
        _, q, _ = candidate(targets[0], bit_count, i)
        rows = pl.ds(pl.multiple_of(q * depth, depth), depth)
        return total + lax.dot_general(stacked[rows, :], mats[i], TN, preferred_element_type=F32)

    start = jnp.zeros((2 * rank, 2 * rank * len(targets)), F32)
    total = lax.fori_loop(0, min(count, 27), step, start)
    result = []
    for l in range(len(targets)):
        part = total[:, 2 * rank * l : 2 * rank * (l + 1)]
        result.append(part[:rank, :rank] + part[rank:, rank:])
    return result


def kernel(
    n,
    panels,
    basis,
    transfer,
    blocks_hbm,
    coupling_hbm,
    near_list,
    out,
    all_panels,
    blocks,
    coupling,
    spread,
    mats0,
    mats1,
    coefs,
    parts,
    clusters,
    blocks_sem,
    coupling_sem,
    panel_send,
    panel_recv,
    coef_send,
    coef_recv,
    relay_send,
    relay_recv,
    part_send,
    part_recv,
    cluster_send,
    cluster_recv,
):
    leaf_dev, columns, points = panels.shape
    rank = basis.shape[1]
    slots = near_list.shape[1]
    half = rank // 2
    low_bits = leaf_dev.bit_length() - 1
    dev_bits = n.bit_length() - 1
    bit_count = low_bits + dev_bits
    group = 8 // leaf_dev
    groups = n // group
    chips = n // 2
    own_rows = leaf_dev * half
    me = lax.axis_index("leaf")
    chip, core = me // 2, me % 2
    mate = chip * 2 + 1 - core

    loads = [pltpu.make_async_copy(coupling_hbm, coupling, coupling_sem)]
    cut = slots // 3 if slots % 3 == 0 else slots
    for l in range(leaf_dev):
        for i in range(slots // cut):
            rows = pl.ds(i * cut, cut)
            loads.append(
                pltpu.make_async_copy(
                    blocks_hbm.at[l, rows],
                    blocks.at[l, rows],
                    blocks_sem.at[l * (slots // cut) + i],
                )
            )
    for load in loads:
        load.start()

    barrier = pltpu.get_barrier_semaphore()

    @pl.loop(1, n)
    def _(j):
        pl.semaphore_signal(
            barrier, inc=1, device_id=(lax.rem(me + j, n),), device_id_type=MESH
        )

    row = lax.broadcasted_iota(jnp.int32, (rank, rank), 0)
    col = lax.broadcasted_iota(jnp.int32, (rank, rank), 1)
    source = 2 * (row % half) + row // half
    order = jnp.where(col == source, 1.0, 0.0).astype(BF16)
    term = jnp.zeros((rank, columns), F32)
    for l in range(leaf_dev):
        flat = lax.dot_general(
            basis[l], panels[l], NT, preferred_element_type=F32
        ).astype(BF16)
        mixed = jnp.dot(order, flat, preferred_element_type=F32).astype(BF16)
        packed = jnp.concatenate([mixed[:half], mixed[half:]], axis=1)
        at = pl.multiple_of(me * own_rows, own_rows) + l * half
        coefs[pl.ds(pl.multiple_of(at, half), half), :] = packed
        sent = lax.dot_general(
            order, transfer[l], NT, preferred_element_type=F32
        ).astype(BF16)
        term = term + jnp.dot(sent, flat, preferred_element_type=F32)
    parts[0] = jnp.concatenate([term[:half], term[half:]], axis=1)
    for l in range(leaf_dev):
        all_panels[me * leaf_dev + l] = panels[l]

    pl.semaphore_wait(barrier, n - 1)

    def own_block(device):
        return coefs.at[pl.ds(pl.multiple_of(device * own_rows, own_rows), own_rows), :]

    places = min(4, chips)
    columns_of_chips = chips // places
    line, place = chip // places, lax.rem(chip, places)

    def coef_device(j, k):
        from_line = lax.rem(line - j + columns_of_chips, columns_of_chips)
        from_place = lax.rem(place - k + places, places)
        return (from_line * places + from_place) * 2 + core

    def coef_copy(j, k):
        to_line = lax.rem(line + j, columns_of_chips) if k is None else line
        to_place = place if k is None else lax.rem(place + k, places)
        m = j * places + (0 if k is None else k)
        block = own_block(me) if k is None else own_block(coef_device(j, 0))
        return pltpu.make_async_remote_copy(
            src_ref=block,
            dst_ref=block,
            send_sem=coef_send.at[m],
            recv_sem=coef_recv.at[m],
            device_id=((to_line * places + to_place) * 2 + core,),
            device_id_type=MESH,
        )

    def relay_copy(m, device):
        return pltpu.make_async_remote_copy(
            src_ref=own_block(device),
            dst_ref=own_block(device),
            send_sem=relay_send.at[m],
            recv_sem=relay_recv.at[m],
            device_id=(mate,),
            device_id_type=MESH,
        )

    def part_copy(j):
        base = (me // group) * group
        return pltpu.make_async_remote_copy(
            src_ref=parts.at[0],
            dst_ref=parts.at[j],
            send_sem=part_send.at[j],
            recv_sem=part_recv.at[j],
            device_id=(base + lax.rem(me - base + j, group),),
            device_id_type=MESH,
        )

    def cluster_block(p):
        return clusters.at[pl.ds(pl.multiple_of(p * half, half), half), :]

    def cluster_copy(j, p):
        return pltpu.make_async_remote_copy(
            src_ref=cluster_block(p),
            dst_ref=cluster_block(p),
            send_sem=cluster_send.at[j],
            recv_sem=cluster_recv.at[j],
            device_id=(lax.rem(me + j * group, n),),
            device_id_type=MESH,
        )

    bits = axis_bits(low_bits, dev_bits)
    where = coords_of(me, bits)

    def hop_of(o):
        x, y, z = OFFSETS[o]
        return (0, y, 0) if y else (x, 0, 0) if x else (0, 0, z)

    def moved(offset):
        there = [where[a] + offset[a] for a in range(3)]
        ok = inside(there, bits)
        return ok, jnp.where(ok, index_of([jnp.maximum(v, 0) for v in there], bits), 0)

    def panel_copy(o, source, receiver):
        first, count = 0, leaf_dev
        if leaf_dev == 2 and OFFSETS[o][0] != 0:
            first, count = (1 if OFFSETS[o][0] > 0 else 0), 1
        rows = pl.ds(source * leaf_dev + first, count)
        owned = hop_of(o) == OFFSETS[o]
        return pltpu.make_async_remote_copy(
            src_ref=panels.at[pl.ds(first, count)] if owned else all_panels.at[rows],
            dst_ref=all_panels.at[rows],
            send_sem=panel_send.at[o],
            recv_sem=panel_recv.at[o],
            device_id=(receiver,),
            device_id_type=MESH,
        )

    def sends(o, act):
        hop = hop_of(o)
        ok, to = moved(hop)
        known, source = moved([h - e for h, e in zip(hop, OFFSETS[o])])

        @pl.when(ok & known)
        def _():
            act(panel_copy(o, source, to))

    def receives(o):
        known, source = moved([-e for e in OFFSETS[o]])

        @pl.when(known)
        def _():
            panel_copy(o, source, me).wait_recv()

    reach = [o for o in range(27) if OFFSETS[o] != (0, 0, 0)]
    along_z = [o for o in reach if not OFFSETS[o][0] and not OFFSETS[o][1]]
    along_x = [o for o in reach if OFFSETS[o][0] and not OFFSETS[o][1]]
    along_y = [o for o in reach if OFFSETS[o][1]]

    def start(copy):
        copy.start()

    for j in range(1, group):
        part_copy(j).start()
    for o in along_z:
        sends(o, start)

    for o in along_x + along_y:
        if hop_of(o) == OFFSETS[o]:
            sends(o, start)

    @pl.loop(1, columns_of_chips)
    def _(j):
        coef_copy(j, None).start()

    relay_copy(0, me).start()
    for k in range(1, places):
        coef_copy(0, k).start()
    for j in range(1, group):
        part_copy(j).wait_recv()
    mine = me // group
    total = parts[0]
    for j in range(1, group):
        total = total + parts[j]
    clusters[pl.ds(pl.multiple_of(mine * half, half), half), :] = total.astype(BF16)

    for o in along_z:
        receives(o)
        for later in along_x + along_y:
            before = [e - h for e, h in zip(OFFSETS[later], hop_of(later))]
            if tuple(before) == OFFSETS[o]:
                sends(later, start)

    @pl.loop(1, columns_of_chips)
    def _(j):
        coef_copy(j, None).wait_recv()
        for k in range(1, places):
            coef_copy(j, k).start()
        relay_copy(j * places, coef_device(j, 0)).start()

    @pl.loop(1, groups)
    def _(j):
        cluster_copy(j, mine).start()

    for o in along_x:
        receives(o)
        for later in along_y:
            before = [e - h for e, h in zip(OFFSETS[later], hop_of(later))]
            if tuple(before) == OFFSETS[o]:
                sends(later, start)

    @pl.loop(0, columns_of_chips)
    def _(j):
        for k in range(1, places):
            coef_copy(j, k).wait_recv()
            relay_copy(j * places + k, coef_device(j, k)).start()

    parent = coords_of(mine, axis_bits(0, bit_count - 3))
    leaf_bits = axis_bits(0, bit_count)
    targets = [coords_of(me * leaf_dev + l, leaf_bits) for l in range(leaf_dev)]
    loads[0].wait()
    far_mats([parent], bit_count - 3, coupling, 1, spread, mats1)
    far_mats(targets, bit_count, coupling, 0, spread, mats0)

    @pl.loop(0, chips)
    def _(m):
        relay_copy(m, me).wait_recv()

    leaf_far = far_sum(targets, bit_count, coefs, mats0, rank)

    @pl.loop(1, groups)
    def _(j):
        cluster_copy(j, mine).wait_recv()

    down = far_sum([parent], bit_count - 3, clusters, mats1, rank)[0].astype(BF16)
    far_terms = []
    for l in range(leaf_dev):
        far = leaf_far[l] + lax.dot_general(down, transfer[l], NT, preferred_element_type=F32)
        far_terms.append(jnp.dot(far.astype(BF16), basis[l], preferred_element_type=F32))

    for o in along_y:
        receives(o)
    for load in loads[1:]:
        load.wait()
    for l in range(leaf_dev):
        total = far_terms[l]
        for k in range(slots):
            j = near_list[l, k]
            block = all_panels[jnp.maximum(j, 0)]
            block = jnp.where(j >= 0, block, jnp.zeros_like(block))
            total = total + jnp.dot(block, blocks[l, k], preferred_element_type=F32)
        out[l] = total.astype(BF16)

    for j in range(1, group):
        part_copy(j).wait_send()

    @pl.loop(0, chips)
    def _(m):
        relay_copy(m, me).wait_send()

    @pl.loop(1, columns_of_chips)
    def _(j):
        coef_copy(j, None).wait_send()

    @pl.loop(0, columns_of_chips)
    def _(j):
        for k in range(1, places):
            coef_copy(j, k).wait_send()

    @pl.loop(1, groups)
    def _(j):
        cluster_copy(j, mine).wait_send()

    for o in reach:
        sends(o, lambda copy: copy.wait_send())


def per_device(panels, basis, transfer, near_blocks, coupling, near_list):
    n = lax.axis_size("leaf")
    leaf_dev, columns, points = panels.shape
    rank = basis.shape[1]
    slots = near_list.shape[1]
    shifts = coupling.shape[1]
    half = rank // 2
    leaves = n * leaf_dev
    coupling = coupling.transpose(1, 0, 2).reshape(shifts, 2, half, 2 * rank)
    coupling = coupling.transpose(0, 2, 1, 3).reshape(shifts, rank, 2 * rank)
    group = 8 // leaf_dev
    vmem = pl.BlockSpec(memory_space=pltpu.VMEM)
    hbm = pl.BlockSpec(memory_space=pl.ANY)
    dma = pltpu.SemaphoreType.DMA
    return pl.pallas_call(
        functools.partial(kernel, n),
        out_shape=jax.ShapeDtypeStruct(panels.shape, BF16),
        in_specs=[vmem, vmem, vmem, hbm, hbm, pl.BlockSpec(memory_space=pltpu.SMEM)],
        out_specs=vmem,
        scratch_shapes=[
            pltpu.VMEM((leaves, columns, points), BF16),
            pltpu.VMEM(near_blocks.shape, BF16),
            pltpu.VMEM(coupling.shape, BF16),
            pltpu.VMEM((leaf_dev * 8 * rank, 2 * rank), F32),
            pltpu.VMEM((min(leaves // 8, 27), 8 * half, 2 * rank * leaf_dev), BF16),
            pltpu.VMEM((min(leaves // 64, 27), 8 * half, 2 * rank), BF16),
            pltpu.VMEM((leaves * half, 2 * columns), BF16),
            pltpu.VMEM((group, half, 2 * columns), F32),
            pltpu.VMEM((n // group * half, 2 * columns), BF16),
            dma((leaf_dev * 3,)),
            dma,
            dma((27,)),
            dma((27,)),
            dma((n // 2,)),
            dma((n // 2,)),
            dma((n // 2,)),
            dma((n // 2,)),
            dma((group,)),
            dma((group,)),
            dma((n // group,)),
            dma((n // group,)),
        ],
        compiler_params=pltpu.CompilerParams(
            collective_id=0, has_side_effects=True, vmem_limit_bytes=60 * 2**20
        ),
    )(panels, basis, transfer, near_blocks, coupling, near_list)


def solution(mesh):
    placed = (
        P("leaf", None, None),
        P("leaf", None, None),
        P("leaf", None, None),
        P("leaf", None, None, None),
        P(),
        P("leaf", None),
    )
    return jax.shard_map(
        per_device, mesh=mesh, in_specs=placed, out_specs=P("leaf", None, None), check_vma=False
    )
```
